32 devices in a mesh: data: 4 (over y, z), tp: 8 (over x, core).
Axes of the slice: x: 4, y: 2, z: 2, core: 2. Of those that a mesh axis runs over, the one named last changes fastest.
The devices are a block of a 4x4x8 slice.
Arguments:
- x_in: bfloat16 [32768, 1536], P('data'), parts along dimension 0
- w_gate: bfloat16 [1536, 8960], P(None, 'tp')
- w_up: bfloat16 [1536, 8960], P(None, 'tp')
- w_down: bfloat16 [8960, 1536], P('tp')
- residual: bfloat16 [32768, 1536], P(('data', 'tp')), parts along dimension 0
- norm_gain: float32 [1536], replicated
Outputs:
- output 1: bfloat16 [32768, 1536], P(('data', 'tp')), parts along dimension 0
- output 2: bfloat16 [32768, 1536], P(('data', 'tp')), parts along dimension 0
There are 4 independent parts. The reference program is written for one: setup_inputs(seed, part) draws one part's arguments, and reference() takes and returns one part's arrays. A program takes and returns all parts, laid end to end along the dimension named above; an argument that names none is the same for every part.
All inputs are finite; a program needn't handle non-finite values.
Results may differ from the reference program's by a relative error of at most 0.00648195.
Values are sent between devices in bfloat16 or wider.
A program may use at most 768 MiB of HBM per device.

```python
import jax
import jax.numpy as jnp
from jax import lax

T = 8192
D = 1536
F = 8960
TP = 8
F_SHARD = F // TP
EPS = 1e-5


def setup_inputs(seed: int = 0, part: int = 0) -> dict:
    key = jax.random.key(seed)
    shared = jax.random.split(key, 4)
    local = jax.random.split(jax.random.fold_in(key, part), 2)
    x_in = jax.random.normal(local[0], (T, D), jnp.float32).astype(jnp.bfloat16)
    residual = jax.random.normal(local[1], (T, D), jnp.float32).astype(jnp.bfloat16)
    w_gate = (jax.random.normal(shared[0], (D, F), jnp.float32) * D ** -0.5).astype(jnp.bfloat16)
    w_up = (jax.random.normal(shared[1], (D, F), jnp.float32) * D ** -0.5).astype(jnp.bfloat16)
    w_down = (jax.random.normal(shared[2], (F, D), jnp.float32) * (2.0 / F) ** 0.5).astype(jnp.bfloat16)
    norm_gain = 1.0 + 0.3 * jax.random.normal(shared[3], (D,), jnp.float32)
    return {"x_in": x_in, "w_gate": w_gate, "w_up": w_up, "w_down": w_down, "residual": residual, "norm_gain": norm_gain}


def reference(x_in, w_gate, w_up, w_down, residual, norm_gain):
    gate_shards = w_gate.reshape(D, TP, F_SHARD).transpose(1, 0, 2)
    up_shards = w_up.reshape(D, TP, F_SHARD).transpose(1, 0, 2)
    down_shards = w_down.reshape(TP, F_SHARD, D)

    def add_shard(running, shard_w):
        gate_cols, up_cols, down_rows = shard_w
        gate_val = jnp.dot(x_in, gate_cols, preferred_element_type=jnp.float32)
        up_val = jnp.dot(x_in, up_cols, preferred_element_type=jnp.float32)
        hidden = (jax.nn.silu(gate_val) * up_val).astype(jnp.bfloat16)
        part_prod = jnp.dot(hidden, down_rows, preferred_element_type=jnp.float32).astype(jnp.bfloat16)
        return running + part_prod.astype(jnp.float32), None

    y_sum = lax.scan(add_shard, jnp.zeros((T, D), jnp.float32), (gate_shards, up_shards, down_shards))[0]
    hidden_sum = residual.astype(jnp.float32) + y_sum
    mean_sq = jnp.mean(hidden_sum * hidden_sum, axis=-1, keepdims=True)
    normed = hidden_sum * lax.rsqrt(mean_sq + EPS) * norm_gain
    return hidden_sum.astype(jnp.bfloat16), normed.astype(jnp.bfloat16)
```

```python
import functools

import jax
import jax.numpy as jnp
from jax import lax
from jax.experimental import pallas as pl
from jax.experimental.pallas import tpu as pltpu
from jax.sharding import PartitionSpec as P

EPS = 1e-5
MESH = pl.DeviceIdType.MESH
TILE = 256
LANE = 128


def dot_nt(a, b):
    return lax.dot_general(a, b, (((1,), (1,)), ((), ())), preferred_element_type=jnp.float32)


def mlp_kernel(
    tp, x_hbm, wg_hbm, wu_hbm, wd_hbm, res_hbm, gain_ref, h_ref, n_ref,
    wg, wu, wt, wd, xbuf, gbuf, dsend, drecv, rrecv, res, hsum,
    w_sem, x_sem, res_sem, ds_sem, dr_sem, rs_sem, rr_sem,
):
    rows = res_hbm.shape[0]
    width = res_hbm.shape[1]
    hid = wg_hbm.shape[0]
    main = hid // LANE * LANE
    tail = hid - main
    chips = tp // 2
    subs = rows // TILE
    sends = (chips - 1) * subs
    total = chips * subs

    me = lax.axis_index("tp")
    chip, core = me // 2, lax.rem(me, 2)
    step_dir = 1 - 2 * core
    partner = me + step_dir
    ahead = 2 * lax.rem(chip + step_dir + chips, chips) + core
    behind = 2 * lax.rem(chip - step_dir + chips, chips) + core

    def my_dest(s):
        return 2 * lax.rem(chip - s * step_dir + 2 * chips, chips) + core

    def partner_dest(s):
        return 2 * lax.rem(chip + s * step_dir + 2 * chips, chips) + (1 - core)

    def x_copy(t, which, slot):
        s, j = t // subs + 1, lax.rem(t, subs)
        dest = my_dest(s) if which else partner_dest(s)
        start = pl.multiple_of(dest * rows + j * TILE, TILE)
        return pltpu.make_async_copy(x_hbm.at[pl.ds(start, TILE), :], xbuf.at[slot, which], x_sem.at[slot, which])

    x_copy(0, 0, 0).start()
    w_copies = [
        pltpu.make_async_copy(wg_hbm.at[pl.ds(0, main), :], wg, w_sem.at[0]),
        pltpu.make_async_copy(wu_hbm.at[pl.ds(0, main), :], wu, w_sem.at[1]),
        pltpu.make_async_copy(wg_hbm.at[pl.ds(main, tail), :], wt.at[pl.ds(0, tail), :], w_sem.at[2]),
        pltpu.make_async_copy(wu_hbm.at[pl.ds(main, tail), :], wt.at[pl.ds(LANE, tail), :], w_sem.at[3]),
        pltpu.make_async_copy(wd_hbm, wd.at[pl.ds(0, hid), :], w_sem.at[4]),
    ]
    for copy in w_copies:
        copy.start()
    x_copy(0, 1, 0).start()
    res_copy = pltpu.make_async_copy(res_hbm, res, res_sem)
    res_copy.start()

    barrier = pltpu.get_barrier_semaphore()
    for peer in (partner, ahead, behind):
        pl.semaphore_signal(barrier, inc=1, device_id={"tp": peer}, device_id_type=MESH)
    pl.semaphore_wait(barrier, 3)

    pad = jnp.zeros((LANE - tail, width), wd.dtype)
    wt[pl.ds(tail, LANE - tail), :] = pad
    wt[pl.ds(LANE + tail, LANE - tail), :] = pad
    wd[pl.ds(hid, LANE - tail), :] = pad
    rrecv[sends] = jnp.zeros(rrecv.shape[1:], rrecv.dtype)
    for copy in w_copies:
        copy.wait()

    def gated(gate_val, up_val):
        return (jax.nn.silu(gate_val) * up_val).astype(jnp.bfloat16)

    def hidden(x_ref):
        x = x_ref[...]
        for c in range(0, main, 256):
            gate_val = dot_nt(x, wg[c:c + 256, :])
            up_val = dot_nt(x, wu[c:c + 256, :])
            gbuf[:, c:c + 256] = gated(gate_val, up_val)
        both = dot_nt(x, wt[...])
        gbuf[:, main:main + LANE] = gated(both[:, :LANE], both[:, LANE:])

    def down(c, n):
        y = jnp.dot(gbuf[...], wd[:, c:c + n], preferred_element_type=jnp.float32)
        return y.astype(jnp.bfloat16)

    def d2d_copy(t):
        slot = lax.rem(t, 2)
        return pltpu.make_async_remote_copy(
            src_ref=dsend.at[slot], dst_ref=drecv.at[t], send_sem=ds_sem.at[slot], recv_sem=dr_sem.at[t],
            device_id={"tp": partner}, device_id_type=MESH,
        )

    def ring_copy(t):
        return pltpu.make_async_remote_copy(
            src_ref=drecv.at[t], dst_ref=rrecv.at[t], send_sem=rs_sem.at[t], recv_sem=rr_sem.at[t],
            device_id={"tp": ahead}, device_id_type=MESH,
        )

    step_n = 512

    def for_partner(t, slot):
        x_copy(t, 0, slot).wait()

        @pl.when(t >= 2)
        def _():
            d2d_copy(t).wait_send()

        hidden(xbuf.at[slot, 0])
        out = dsend.at[lax.rem(t, 2)]
        for c in range(0, width, step_n):
            out[:, c:c + step_n] = down(c, step_n)
        d2d_copy(t).start()

    def prefetch(t, slot):
        @pl.when(t + 1 < total)
        def _():
            x_copy(t + 1, 0, 1 - slot).start()
            x_copy(t + 1, 1, 1 - slot).start()

    def send_step(t, carry):
        slot = lax.rem(t, 2)
        prefetch(t, slot)
        for_partner(t, slot)
        x_copy(t, 1, slot).wait()
        hidden(xbuf.at[slot, 1])
        d2d_copy(t).wait_recv()

        @pl.when(t >= subs)
        def _():
            ring_copy(t - subs).wait_recv()

        older = jnp.where(t >= subs, t - subs, sends)
        for c in range(0, width, step_n):
            own = down(c, step_n).astype(jnp.float32)
            both = own + drecv[t, :, c:c + step_n].astype(jnp.float32)
            both = both + rrecv[older, :, c:c + step_n].astype(jnp.float32)
            drecv[t, :, c:c + step_n] = both.astype(jnp.bfloat16)
        ring_copy(t).start()
        return carry

    def last_step(t, carry):
        slot = lax.rem(t, 2)
        j = t - sends
        prefetch(t, slot)
        for_partner(t, slot)
        x_copy(t, 1, slot).wait()
        hidden(xbuf.at[slot, 1])
        d2d_copy(t).wait_recv()
        for c in range(0, width, step_n):
            own = down(c, step_n).astype(jnp.float32)
            hsum[:, c:c + step_n] = own + drecv[t, :, c:c + step_n].astype(jnp.float32)
        ring_copy(t - subs).wait_recv()

        def finish(r, carry):
            at = pl.ds(pl.multiple_of(r * 16, 16), 16)
            h = hsum[at, :] + rrecv[t - subs, at, :].astype(jnp.float32)
            h = res[pl.ds(pl.multiple_of(j * TILE + r * 16, 16), 16), :].astype(jnp.float32) + h
            mean_sq = jnp.mean(h * h, axis=-1, keepdims=True)
            out_at = pl.ds(pl.multiple_of(j * TILE + r * 16, 16), 16)
            h_ref[out_at, :] = h.astype(jnp.bfloat16)
            n_ref[out_at, :] = (h * lax.rsqrt(mean_sq + EPS) * gain_ref[...]).astype(jnp.bfloat16)
            return carry

        lax.fori_loop(0, TILE // 16, finish, 0, unroll=4)
        return carry

    lax.fori_loop(0, sends, send_step, 0)
    res_copy.wait()
    lax.fori_loop(sends, total, last_step, 0)

    for t in (total - 2, total - 1):
        d2d_copy(t).wait_send()
    for t in range(sends):
        ring_copy(t).wait_send()


def solution(mesh):
    tp = mesh.shape["tp"]

    def local_block(x_in, w_gate, w_up, w_down, residual, norm_gain):
        rows, width = residual.shape
        hid = w_gate.shape[1]
        padded = hid // LANE * LANE + LANE
        chips, subs = tp // 2, rows // TILE
        sends, total = (chips - 1) * subs, chips * subs
        bf16 = jnp.bfloat16
        any_spec = pl.BlockSpec(memory_space=pl.ANY)
        vmem_spec = pl.BlockSpec(memory_space=pltpu.VMEM)
        out = jax.ShapeDtypeStruct((rows, width), bf16)
        flops = 6 * x_in.shape[0] * width * hid
        return pl.pallas_call(
            functools.partial(mlp_kernel, tp),
            out_shape=(out, out),
            in_specs=[any_spec] * 5 + [vmem_spec],
            out_specs=(vmem_spec, vmem_spec),
            scratch_shapes=[
                pltpu.VMEM((padded - LANE, width), bf16),
                pltpu.VMEM((padded - LANE, width), bf16),
                pltpu.VMEM((2 * LANE, width), bf16),
                pltpu.VMEM((padded, width), bf16),
                pltpu.VMEM((2, 2, TILE, width), bf16),
                pltpu.VMEM((TILE, padded), bf16),
                pltpu.VMEM((2, TILE, width), bf16),
                pltpu.VMEM((total, TILE, width), bf16),
                pltpu.VMEM((sends + 1, TILE, width), bf16),
                pltpu.VMEM((rows, width), bf16),
                pltpu.VMEM((TILE, width), jnp.float32),
                pltpu.SemaphoreType.DMA((5,)),
                pltpu.SemaphoreType.DMA((2, 2)),
                pltpu.SemaphoreType.DMA,
                pltpu.SemaphoreType.DMA((2,)),
                pltpu.SemaphoreType.DMA((total,)),
                pltpu.SemaphoreType.DMA((sends,)),
                pltpu.SemaphoreType.DMA((sends,)),
            ],
            compiler_params=pltpu.CompilerParams(
                collective_id=0, has_side_effects=True, vmem_limit_bytes=56 * 2**20,
            ),
            cost_estimate=pl.CostEstimate(flops=flops, bytes_accessed=2 * x_in.size, transcendentals=0),
        )(x_in, w_gate.T, w_up.T, w_down, residual, norm_gain.reshape(1, width))

    row_spec = P(("data", "tp"), None)
    return jax.shard_map(
        local_block,
        mesh=mesh,
        in_specs=(P("data", None), P(None, "tp"), P(None, "tp"), P("tp", None), row_spec, P(None)),
        out_specs=(row_spec, row_spec),
        check_vma=False,
    )
```

```python
import functools

import jax
import jax.numpy as jnp
from jax import lax
from jax.experimental import pallas as pl
from jax.experimental.pallas import tpu as pltpu
from jax.sharding import PartitionSpec as P

EPS = 1e-5
MESH = pl.DeviceIdType.MESH
TILE = 128
LANE = 128
STEP = 256
COLS = 512
ROWS = 16


def dot_nt(a, b):
    return lax.dot_general(a, b, (((1,), (1,)), ((), ())), preferred_element_type=jnp.float32)


def gated(gate_val, up_val):
    return (jax.nn.silu(gate_val) * up_val).astype(jnp.bfloat16)


def mlp_kernel(
    tp, x_hbm, wg_hbm, wu_hbm, wd_hbm, res_hbm, gain_ref, h_ref, n_ref,
    wg, wu, wt, wt_t, wd, xbuf, gbuf, own, dsend, drecv, rrecv, res,
    w_sem, x_sem, res_sem, ds_sem, dr_sem, rs_sem, rr_sem,
):
    rows, width = res_hbm.shape
    hid = wg_hbm.shape[0]
    main = hid // LANE * LANE
    tail = hid - main
    chips = tp // 2
    subs = rows // TILE
    sends = (chips - 1) * subs
    total = chips * subs

    me = lax.axis_index("tp")
    chip, core = me // 2, lax.rem(me, 2)
    step_dir = 1 - 2 * core
    partner = me + step_dir
    ahead = 2 * lax.rem(chip + step_dir + chips, chips) + core
    behind = 2 * lax.rem(chip - step_dir + chips, chips) + core

    def x_copies(t, slot):
        s, j = t // subs + 1, lax.rem(t, subs)
        theirs = 2 * lax.rem(chip + s * step_dir + 2 * chips, chips) + (1 - core)
        mine = 2 * lax.rem(chip - s * step_dir + 2 * chips, chips) + core
        return [
            pltpu.make_async_copy(
                x_hbm.at[pl.ds(pl.multiple_of(dest * rows + j * TILE, TILE), TILE), :],
                xbuf.at[slot, pl.ds(i * TILE, TILE), :],
                x_sem.at[slot, i],
            )
            for i, dest in enumerate((theirs, mine))
        ]

    def d2d_copy(t):
        slot = lax.rem(t, 2)
        return pltpu.make_async_remote_copy(
            src_ref=dsend.at[slot], dst_ref=drecv.at[t], send_sem=ds_sem.at[slot], recv_sem=dr_sem.at[t],
            device_id={"tp": partner}, device_id_type=MESH,
        )

    def ring_copy(t):
        return pltpu.make_async_remote_copy(
            src_ref=drecv.at[t], dst_ref=rrecv.at[t], send_sem=rs_sem.at[t], recv_sem=rr_sem.at[t],
            device_id={"tp": ahead}, device_id_type=MESH,
        )

    for copy in x_copies(0, 0):
        copy.start()
    last = main // STEP
    tail_loads = [
        pltpu.make_async_copy(wg_hbm.at[pl.ds(main, tail), :], wt.at[pl.ds(0, tail), :], w_sem.at[0, last]),
        pltpu.make_async_copy(wu_hbm.at[pl.ds(main, tail), :], wt.at[pl.ds(LANE, tail), :], w_sem.at[1, last]),
    ]
    for copy in tail_loads:
        copy.start()
    up_steps = [(c, min(STEP, main - c)) for c in range(0, main, STEP)]
    gate_loads, up_loads = [], []
    for i, (c, n) in enumerate(up_steps):
        gate_loads.append(pltpu.make_async_copy(wg_hbm.at[pl.ds(c, n), :], wg.at[pl.ds(c, n), :], w_sem.at[0, i]))
        up_loads.append(pltpu.make_async_copy(wu_hbm.at[pl.ds(c, n), :], wu.at[pl.ds(c, n), :], w_sem.at[1, i]))
    down_loads = [
        pltpu.make_async_copy(wd_hbm.at[:, pl.ds(c, COLS)], wd.at[pl.ds(0, hid), pl.ds(c, COLS)], w_sem.at[2, i])
        for i, c in enumerate(range(0, width, COLS))
    ]
    res_copy = pltpu.make_async_copy(res_hbm, res, res_sem)
    half = len(up_steps) // 2
    for copy in gate_loads[:half] + up_loads[:half]:
        copy.start()

    barrier = pltpu.get_barrier_semaphore()
    for peer in (partner, ahead, behind):
        pl.semaphore_signal(barrier, inc=1, device_id={"tp": peer}, device_id_type=MESH)

    pad = jnp.zeros((LANE - tail, width), wd.dtype)
    wt[pl.ds(tail, LANE - tail), :] = pad
    wt[pl.ds(LANE + tail, LANE - tail), :] = pad
    wd[pl.ds(hid, LANE - tail), :] = pad

    def hidden_step(t, c, n):
        x = xbuf[lax.rem(t, 2)]
        gbuf[lax.rem(t, 2), :, c:c + n] = gated(dot_nt(x, wg[c:c + n, :]), dot_nt(x, wu[c:c + n, :]))

    def hidden_tail(t):
        for i in range(2):
            at = pl.ds(i * TILE, TILE)
            both = jnp.dot(xbuf[lax.rem(t, 2), at, :], wt_t[...], preferred_element_type=jnp.float32)
            gbuf[lax.rem(t, 2), at, main:main + LANE] = gated(both[:, :LANE], both[:, LANE:])

    def down_step(t, c):
        g = gbuf[lax.rem(t, 2)]
        y = jnp.dot(g, wd[:, c:c + COLS], preferred_element_type=jnp.float32).astype(jnp.bfloat16)
        dsend[lax.rem(t, 2), :, c:c + COLS] = y[:TILE]
        own[lax.rem(t, subs), :, c:c + COLS] = y[TILE:]

    def down_rows(t, c, i):
        g = gbuf[lax.rem(t, 2), pl.ds(i * TILE, TILE), :]
        y = jnp.dot(g, wd[:, c:c + COLS], preferred_element_type=jnp.float32).astype(jnp.bfloat16)
        if i == 0:
            dsend[lax.rem(t, 2), :, c:c + COLS] = y
        else:
            own[lax.rem(t, subs), :, c:c + COLS] = y

    def combine(t, first, part=0, parts=1):
        for r in range(part * TILE // parts, (part + 1) * TILE // parts, ROWS):
            for c in range(0, width, COLS):
                at = (pl.ds(r, ROWS), slice(c, c + COLS))
                both = own[lax.rem(t, subs), *at].astype(jnp.float32) + drecv[t, *at].astype(jnp.float32)
                if not first:
                    both = both + rrecv[t - subs, *at].astype(jnp.float32)
                drecv[t, *at] = both.astype(jnp.bfloat16)

    def finish_rows(j, r):
        at = pl.ds(r, ROWS)
        out_at = pl.ds(pl.multiple_of(j * TILE + r, ROWS), ROWS)
        y = own[j, at, :].astype(jnp.float32) + drecv[sends + j, at, :].astype(jnp.float32)
        y = y + rrecv[sends - subs + j, at, :].astype(jnp.float32)
        h = res[out_at, :].astype(jnp.float32) + y
        mean_sq = jnp.mean(h * h, axis=-1, keepdims=True)
        h_ref[out_at, :] = h.astype(jnp.bfloat16)
        n_ref[out_at, :] = (h * lax.rsqrt(mean_sq + EPS) * gain_ref[...].reshape(1, width)).astype(jnp.bfloat16)

    def wait_last(j):
        d2d_copy(sends + j).wait_recv()
        ring_copy(sends - subs + j).wait_recv()

    def early_tile(t, with_sum=True):
        for copy in x_copies(t + 2, lax.rem(t, 2)):
            copy.start()
        for copy in x_copies(t + 1, lax.rem(t + 1, 2)):
            copy.wait()

        if with_sum:
            d2d_copy(t).wait_send()
        if with_sum:
            d2d_copy(t - 1).wait_recv()
            combine(t - 1, True)
            ring_copy(t - 1).start()
        for c in range(0, width, COLS):
            down_step(t, c)
        d2d_copy(t).start()
        for c, n in up_steps:
            hidden_step(t + 1, c, n)
        hidden_tail(t + 1)

    def tile(t, with_sum, with_end):
        @pl.when(t + 2 < total)
        def _():
            for copy in x_copies(t + 2, lax.rem(t, 2)):
                copy.start()

        for copy in x_copies(t + 1, lax.rem(t + 1, 2)):
            copy.wait()
        d2d_copy(t).wait_send()
        if with_sum:
            d2d_copy(t - 2).wait_recv()
            ring_copy(t - 2 - subs).wait_recv()
        if with_end:
            wait_last(t - 2 - sends)
        for c in range(0, width, COLS):
            down_step(t, c)
        parts = len(up_steps)
        for i, (c, n) in enumerate(up_steps):
            hidden_step(t + 1, c, n)
            if with_sum:
                combine(t - 2, False, i, parts)
            if with_end:
                for r in range(i * TILE // parts, (i + 1) * TILE // parts, ROWS):
                    finish_rows(t - 2 - sends, r)
        hidden_tail(t + 1)
        if with_sum:
            ring_copy(t - 2).start()
        d2d_copy(t).start()

    for copy in x_copies(0, 0):
        copy.wait()
    for copy in tail_loads:
        copy.wait()
    for copy in gate_loads[half:] + up_loads[half:]:
        copy.start()
    wt_t[...] = wt[...].T
    hidden_tail(0)
    for part in (range(half), range(half, len(up_steps))):
        for i in part:
            gate_loads[i].wait()
            up_loads[i].wait()
        if not part[0]:
            for copy in down_loads:
                copy.start()
        for i in part:
            hidden_step(0, *up_steps[i])
    for copy in x_copies(1, 1):
        copy.start()
    for copy in down_loads:
        copy.wait()
    pl.semaphore_wait(barrier, 3)
    for c in range(0, width, COLS):
        down_rows(0, c, 0)
    d2d_copy(0).start()
    for copy in x_copies(2, 0):
        copy.start()
    for copy in x_copies(1, 1):
        copy.wait()
    for c in range(0, width, COLS):
        down_rows(0, c, 1)
    for c, n in up_steps[:half]:
        hidden_step(1, c, n)
    res_copy.start()
    d2d_copy(0).wait_recv()
    combine(0, True)
    ring_copy(0).start()
    for c, n in up_steps[half:]:
        hidden_step(1, c, n)
    hidden_tail(1)

    def early(t, carry):
        early_tile(t)
        return carry

    def with_sum(t, carry):
        tile(t, True, False)
        return carry

    def with_end(t, carry):
        tile(t, False, True)
        return carry

    early_tile(1, False)
    lax.fori_loop(2, subs + 1, early, 0)
    tile(subs + 1, False, False)
    lax.fori_loop(subs + 2, sends + 2, with_sum, 0)
    res_copy.wait()
    lax.fori_loop(sends + 2, total - 1, with_end, 0)
    d2d_copy(total - 1).wait_send()
    for c in range(0, width, COLS):
        down_step(total - 1, c)
    d2d_copy(total - 1).start()

    def finish_tile(j, carry):
        wait_last(j)
        for r in range(0, TILE, ROWS):
            finish_rows(j, r)
        return carry

    lax.fori_loop(total - 3 - sends, subs, finish_tile, 0)

    for t in (total - 2, total - 1):
        d2d_copy(t).wait_send()
    for t in range(sends):
        ring_copy(t).wait_send()


def store_kernel(h_ref, n_ref, h_hbm, n_hbm, sem):
    rows = h_ref.shape[0] // 4
    copies = [
        pltpu.make_async_copy(src.at[pl.ds(i * rows, rows), :], dst.at[pl.ds(i * rows, rows), :], sem.at[k, i])
        for i in range(4)
        for k, (src, dst) in enumerate(((h_ref, h_hbm), (n_ref, n_hbm)))
    ]
    for copy in copies:
        copy.start()
    for copy in copies:
        copy.wait()


def solution(mesh):
    tp = mesh.shape["tp"]

    def local_block(x_in, w_gate, w_up, w_down, residual, norm_gain):
        rows, width = residual.shape
        hid = w_gate.shape[1]
        main = hid // LANE * LANE
        padded = main + LANE
        chips, subs = tp // 2, rows // TILE
        sends, total = (chips - 1) * subs, chips * subs
        bf16 = jnp.bfloat16
        any_spec = pl.BlockSpec(memory_space=pl.ANY)
        vmem_spec = pl.BlockSpec(memory_space=pltpu.VMEM)
        out = pltpu.VMEM((rows, width), bf16)
        flops = 6 * x_in.shape[0] * width * hid
        h_out, n_out = pl.pallas_call(
            functools.partial(mlp_kernel, tp),
            out_shape=(out, out),
            in_specs=[any_spec] * 5 + [vmem_spec],
            out_specs=(vmem_spec, vmem_spec),
            scratch_shapes=[
                pltpu.VMEM((main, width), bf16),
                pltpu.VMEM((main, width), bf16),
                pltpu.VMEM((2 * LANE, width), bf16),
                pltpu.VMEM((width, 2 * LANE), bf16),
                pltpu.VMEM((padded, width), bf16),
                pltpu.VMEM((2, 2 * TILE, width), bf16),
                pltpu.VMEM((2, 2 * TILE, padded), bf16),
                pltpu.VMEM((subs, TILE, width), bf16),
                pltpu.VMEM((2, TILE, width), bf16),
                pltpu.VMEM((total, TILE, width), bf16),
                pltpu.VMEM((sends, TILE, width), bf16),
                pltpu.VMEM((rows, width), bf16),
                pltpu.SemaphoreType.DMA((3, main // STEP + 2)),
                pltpu.SemaphoreType.DMA((2, 2)),
                pltpu.SemaphoreType.DMA,
                pltpu.SemaphoreType.DMA((2,)),
                pltpu.SemaphoreType.DMA((total,)),
                pltpu.SemaphoreType.DMA((sends,)),
                pltpu.SemaphoreType.DMA((sends,)),
            ],
            compiler_params=pltpu.CompilerParams(
                collective_id=0, has_side_effects=True, vmem_limit_bytes=56 * 2**20,
            ),
            cost_estimate=pl.CostEstimate(flops=flops, bytes_accessed=2 * x_in.size, transcendentals=0),
        )(x_in, w_gate.T, w_up.T, w_down, residual, norm_gain)
        stored = jax.ShapeDtypeStruct((rows, width), bf16)
        return pl.pallas_call(
            store_kernel,
            out_shape=(stored, stored),
            in_specs=[vmem_spec, vmem_spec],
            out_specs=(any_spec, any_spec),
            scratch_shapes=[pltpu.SemaphoreType.DMA((2, 4))],
            compiler_params=pltpu.CompilerParams(vmem_limit_bytes=2**20),
        )(pltpu.with_memory_space_constraint(h_out, pltpu.VMEM), pltpu.with_memory_space_constraint(n_out, pltpu.VMEM))

    row_spec = P(("data", "tp"), None)
    return jax.shard_map(
        local_block,
        mesh=mesh,
        in_specs=(P("data", None), P(None, "tp"), P(None, "tp"), P("tp", None), row_spec, P(None)),
        out_specs=(row_spec, row_spec),
        check_vma=False,
    )
```

```python
import functools

import jax
import jax.numpy as jnp
from jax import lax
from jax.experimental import pallas as pl
from jax.experimental.pallas import tpu as pltpu
from jax.sharding import PartitionSpec as P

EPS = 1e-5
MESH = pl.DeviceIdType.MESH
TILE = 128
LANE = 128
STEP = 256
COLS = 512
ROWS = 16


def dot_nt(a, b):
    return lax.dot_general(a, b, (((1,), (1,)), ((), ())), preferred_element_type=jnp.float32)


def gated(gate_val, up_val):
    return (jax.nn.silu(gate_val) * up_val).astype(jnp.bfloat16)


def mlp_kernel(
    tp, x_hbm, wg_hbm, wu_hbm, wd_hbm, res_hbm, gain_ref, h_ref, n_ref,
    wg, wu, wt, wt_t, wd, xbuf, gbuf, own, dsend, drecv, rrecv, res,
    w_sem, x_sem, res_sem, ds_sem, dr_sem, rs_sem, rr_sem,
):
    rows, width = res_hbm.shape
    hid = wg_hbm.shape[0]
    main = hid // LANE * LANE
    tail = hid - main
    chips = tp // 2
    subs = rows // TILE
    sends = (chips - 1) * subs
    total = chips * subs

    me = lax.axis_index("tp")
    chip, core = me // 2, lax.rem(me, 2)
    step_dir = 1 - 2 * core
    partner = me + step_dir
    ahead = 2 * lax.rem(chip + step_dir + chips, chips) + core
    behind = 2 * lax.rem(chip - step_dir + chips, chips) + core

    def x_copies(t, slot):
        s, j = t // subs + 1, lax.rem(t, subs)
        theirs = 2 * lax.rem(chip + s * step_dir + 2 * chips, chips) + (1 - core)
        mine = 2 * lax.rem(chip - s * step_dir + 2 * chips, chips) + core
        return [
            pltpu.make_async_copy(
                x_hbm.at[pl.ds(pl.multiple_of(dest * rows + j * TILE, TILE), TILE), :],
                xbuf.at[slot, pl.ds(i * TILE, TILE), :],
                x_sem.at[slot, i],
            )
            for i, dest in enumerate((theirs, mine))
        ]

    def d2d_copy(t):
        slot = lax.rem(t, 2)
        return pltpu.make_async_remote_copy(
            src_ref=dsend.at[slot], dst_ref=drecv.at[t], send_sem=ds_sem.at[slot], recv_sem=dr_sem.at[t],
            device_id={"tp": partner}, device_id_type=MESH,
        )

    def ring_copy(t):
        return pltpu.make_async_remote_copy(
            src_ref=drecv.at[t], dst_ref=rrecv.at[t], send_sem=rs_sem.at[t], recv_sem=rr_sem.at[t],
            device_id={"tp": ahead}, device_id_type=MESH,
        )

    for copy in x_copies(0, 0):
        copy.start()
    last = main // STEP
    tail_loads = [
        pltpu.make_async_copy(wg_hbm.at[pl.ds(main, tail), :], wt.at[pl.ds(0, tail), :], w_sem.at[0, last]),
        pltpu.make_async_copy(wu_hbm.at[pl.ds(main, tail), :], wt.at[pl.ds(LANE, tail), :], w_sem.at[1, last]),
    ]
    for copy in tail_loads:
        copy.start()
    up_steps = [(c, min(STEP, main - c)) for c in range(0, main, STEP)]
    gate_loads, up_loads = [], []
    for i, (c, n) in enumerate(up_steps):
        gate_loads.append(pltpu.make_async_copy(wg_hbm.at[pl.ds(c, n), :], wg.at[pl.ds(c, n), :], w_sem.at[0, i]))
        up_loads.append(pltpu.make_async_copy(wu_hbm.at[pl.ds(c, n), :], wu.at[pl.ds(c, n), :], w_sem.at[1, i]))
    down_loads = [pltpu.make_async_copy(wd_hbm, wd.at[pl.ds(0, hid), :], w_sem.at[2, 0])]
    res_copy = pltpu.make_async_copy(res_hbm, res, res_sem)
    half = len(up_steps) // 2
    for copy in gate_loads[:half] + up_loads[:half]:
        copy.start()

    barrier = pltpu.get_barrier_semaphore()
    for peer in (partner, ahead, behind):
        pl.semaphore_signal(barrier, inc=1, device_id={"tp": peer}, device_id_type=MESH)

    pad = jnp.zeros((LANE - tail, width), wd.dtype)
    wt[pl.ds(tail, LANE - tail), :] = pad
    wt[pl.ds(LANE + tail, LANE - tail), :] = pad
    wd[pl.ds(hid, LANE - tail), :] = pad

    def hidden_step(t, c, n):
        x = xbuf[lax.rem(t, 2)]
        gbuf[lax.rem(t, 2), :, c:c + n] = gated(dot_nt(x, wg[c:c + n, :]), dot_nt(x, wu[c:c + n, :]))

    def hidden_tail(t):
        for i in range(2):
            at = pl.ds(i * TILE, TILE)
            both = jnp.dot(xbuf[lax.rem(t, 2), at, :], wt_t[...], preferred_element_type=jnp.float32)
            gbuf[lax.rem(t, 2), at, main:main + LANE] = gated(both[:, :LANE], both[:, LANE:])

    def down_step(t, c):
        g = gbuf[lax.rem(t, 2)]
        y = jnp.dot(g, wd[:, c:c + COLS], preferred_element_type=jnp.float32).astype(jnp.bfloat16)
        dsend[lax.rem(t, 2), :, c:c + COLS] = y[:TILE]
        own[lax.rem(t, subs), :, c:c + COLS] = y[TILE:]

    def down_rows(t, c, i):
        g = gbuf[lax.rem(t, 2), pl.ds(i * TILE, TILE), :]
        y = jnp.dot(g, wd[:, c:c + COLS], preferred_element_type=jnp.float32).astype(jnp.bfloat16)
        if i == 0:
            dsend[lax.rem(t, 2), :, c:c + COLS] = y
        else:
            own[lax.rem(t, subs), :, c:c + COLS] = y

    def combine(t, first, part=0, parts=1):
        for r in range(part * TILE // parts, (part + 1) * TILE // parts, ROWS):
            for c in range(0, width, COLS):
                at = (pl.ds(r, ROWS), slice(c, c + COLS))
                both = own[lax.rem(t, subs), *at].astype(jnp.float32) + drecv[t, *at].astype(jnp.float32)
                if not first:
                    both = both + rrecv[t - subs, *at].astype(jnp.float32)
                drecv[t, *at] = both.astype(jnp.bfloat16)

    def finish_rows(j, r):
        at = pl.ds(r, ROWS)
        out_at = pl.ds(pl.multiple_of(j * TILE + r, ROWS), ROWS)
        y = own[j, at, :].astype(jnp.float32) + drecv[sends + j, at, :].astype(jnp.float32)
        y = y + rrecv[sends - subs + j, at, :].astype(jnp.float32)
        h = res[out_at, :].astype(jnp.float32) + y
        mean_sq = jnp.mean(h * h, axis=-1, keepdims=True)
        h_ref[out_at, :] = h.astype(jnp.bfloat16)
        n_ref[out_at, :] = (h * lax.rsqrt(mean_sq + EPS) * gain_ref[...].reshape(1, width)).astype(jnp.bfloat16)

    def wait_last(j):
        d2d_copy(sends + j).wait_recv()
        ring_copy(sends - subs + j).wait_recv()

    def early_tile(t, with_sum=True):
        for copy in x_copies(t + 2, lax.rem(t, 2)):
            copy.start()
        for copy in x_copies(t + 1, lax.rem(t + 1, 2)):
            copy.wait()

        d2d_copy(t).wait_send()
        if with_sum:
            d2d_copy(t - 1).wait_recv()
            combine(t - 1, True)
            ring_copy(t - 1).start()
        for c in range(0, width, COLS):
            down_step(t, c)
        d2d_copy(t).start()
        for c, n in up_steps:
            hidden_step(t + 1, c, n)
        hidden_tail(t + 1)

    def tile(t, with_sum, with_end, lag=2):
        @pl.when(t + 2 < total)
        def _():
            for copy in x_copies(t + 2, lax.rem(t, 2)):
                copy.start()

        for copy in x_copies(t + 1, lax.rem(t + 1, 2)):
            copy.wait()
        d2d_copy(t).wait_send()
        if with_sum:
            d2d_copy(t - lag).wait_recv()
            ring_copy(t - lag - subs).wait_recv()
        if with_end:
            wait_last(t - 2 - sends)
        for c in range(0, width, COLS):
            down_step(t, c)
        parts = len(up_steps)
        for i, (c, n) in enumerate(up_steps):
            hidden_step(t + 1, c, n)
            if with_sum:
                combine(t - lag, False, i, parts)
            if with_end:
                for r in range(i * TILE // parts, (i + 1) * TILE // parts, ROWS):
                    finish_rows(t - 2 - sends, r)
        hidden_tail(t + 1)
        if with_sum:
            ring_copy(t - lag).start()
        d2d_copy(t).start()

    for copy in x_copies(0, 0):
        copy.wait()
    for copy in tail_loads:
        copy.wait()
    for copy in gate_loads[half:] + up_loads[half:] + down_loads:
        copy.start()
    wt_t[...] = wt[...].T
    hidden_tail(0)
    for part in (range(half), range(half, len(up_steps))):
        for i in part:
            gate_loads[i].wait()
            up_loads[i].wait()
        for i in part:
            hidden_step(0, *up_steps[i])
    for copy in x_copies(1, 1):
        copy.start()
    for copy in down_loads:
        copy.wait()
    pl.semaphore_wait(barrier, 3)
    for c in range(0, width, COLS):
        down_rows(0, c, 0)
    d2d_copy(0).start()
    for copy in x_copies(2, 0):
        copy.start()
    for copy in x_copies(1, 1):
        copy.wait()
    for c in range(0, width, COLS):
        down_rows(0, c, 1)
    for c, n in up_steps[:half]:
        hidden_step(1, c, n)
    res_copy.start()
    d2d_copy(0).wait_recv()
    combine(0, True)
    ring_copy(0).start()
    for c, n in up_steps[half:]:
        hidden_step(1, c, n)
    hidden_tail(1)

    def early(t, carry):
        early_tile(t)
        return carry

    def with_sum(t, carry):
        tile(t, True, False)
        return carry

    def with_end(t, carry):
        tile(t, False, True)
        return carry

    for copy in x_copies(3, 1):
        copy.start()
    for copy in x_copies(2, 0):
        copy.wait()
    for c in range(0, width, COLS):
        down_rows(1, c, 0)
    d2d_copy(1).start()
    for c in range(0, width, COLS):
        down_rows(1, c, 1)
    for c, n in up_steps[:half]:
        hidden_step(2, c, n)
    d2d_copy(1).wait_recv()
    combine(1, True)
    ring_copy(1).start()
    for c, n in up_steps[half:]:
        hidden_step(2, c, n)
    hidden_tail(2)
    early_tile(2, False)
    lax.fori_loop(3, subs + 1, early, 0)
    tile(subs + 1, True, False, lag=1)
    tile(subs + 2, False, False)
    lax.fori_loop(subs + 3, sends + 2, with_sum, 0)
    res_copy.wait()
    lax.fori_loop(sends + 2, total - 1, with_end, 0)
    d2d_copy(total - 1).wait_send()
    for c in range(0, width, COLS):
        down_step(total - 1, c)
    d2d_copy(total - 1).start()

    def finish_tile(j, carry):
        wait_last(j)
        for r in range(0, TILE, ROWS):
            finish_rows(j, r)
        return carry

    lax.fori_loop(total - 3 - sends, subs, finish_tile, 0)

    for t in (total - 2, total - 1):
        d2d_copy(t).wait_send()
    for t in range(sends):
        ring_copy(t).wait_send()


def store_kernel(h_ref, n_ref, h_hbm, n_hbm, sem):
    rows = h_ref.shape[0] // 2
    copies = [
        pltpu.make_async_copy(src.at[pl.ds(i * rows, rows), :], dst.at[pl.ds(i * rows, rows), :], sem.at[k, i])
        for i in range(2)
        for k, (src, dst) in enumerate(((h_ref, h_hbm), (n_ref, n_hbm)))
    ]
    for copy in copies:
        copy.start()
    for copy in copies:
        copy.wait()


def solution(mesh):
    tp = mesh.shape["tp"]

    def local_block(x_in, w_gate, w_up, w_down, residual, norm_gain):
        rows, width = residual.shape
        hid = w_gate.shape[1]
        main = hid // LANE * LANE
        padded = main + LANE
        chips, subs = tp // 2, rows // TILE
        sends, total = (chips - 1) * subs, chips * subs
        bf16 = jnp.bfloat16
        any_spec = pl.BlockSpec(memory_space=pl.ANY)
        vmem_spec = pl.BlockSpec(memory_space=pltpu.VMEM)
        out = pltpu.VMEM((rows, width), bf16)
        flops = 6 * x_in.shape[0] * width * hid
        h_out, n_out = pl.pallas_call(
            functools.partial(mlp_kernel, tp),
            out_shape=(out, out),
            in_specs=[any_spec] * 5 + [vmem_spec],
            out_specs=(vmem_spec, vmem_spec),
            scratch_shapes=[
                pltpu.VMEM((main, width), bf16),
                pltpu.VMEM((main, width), bf16),
                pltpu.VMEM((2 * LANE, width), bf16),
                pltpu.VMEM((width, 2 * LANE), bf16),
                pltpu.VMEM((padded, width), bf16),
                pltpu.VMEM((2, 2 * TILE, width), bf16),
                pltpu.VMEM((2, 2 * TILE, padded), bf16),
                pltpu.VMEM((subs, TILE, width), bf16),
                pltpu.VMEM((2, TILE, width), bf16),
                pltpu.VMEM((total, TILE, width), bf16),
                pltpu.VMEM((sends, TILE, width), bf16),
                pltpu.VMEM((rows, width), bf16),
                pltpu.SemaphoreType.DMA((3, main // STEP + 2)),
                pltpu.SemaphoreType.DMA((2, 2)),
                pltpu.SemaphoreType.DMA,
                pltpu.SemaphoreType.DMA((2,)),
                pltpu.SemaphoreType.DMA((total,)),
                pltpu.SemaphoreType.DMA((sends,)),
                pltpu.SemaphoreType.DMA((sends,)),
            ],
            compiler_params=pltpu.CompilerParams(
                collective_id=0, has_side_effects=True, vmem_limit_bytes=56 * 2**20,
            ),
            cost_estimate=pl.CostEstimate(flops=flops, bytes_accessed=2 * x_in.size, transcendentals=0),
        )(x_in, w_gate.T, w_up.T, w_down, residual, norm_gain)
        stored = jax.ShapeDtypeStruct((rows, width), bf16)
        return pl.pallas_call(
            store_kernel,
            out_shape=(stored, stored),
            in_specs=[vmem_spec, vmem_spec],
            out_specs=(any_spec, any_spec),
            scratch_shapes=[pltpu.SemaphoreType.DMA((2, 2))],
            compiler_params=pltpu.CompilerParams(vmem_limit_bytes=2**20),
        )(pltpu.with_memory_space_constraint(h_out, pltpu.VMEM), pltpu.with_memory_space_constraint(n_out, pltpu.VMEM))

    row_spec = P(("data", "tp"), None)
    return jax.shard_map(
        local_block,
        mesh=mesh,
        in_specs=(P("data", None), P(None, "tp"), P(None, "tp"), P("tp", None), row_spec, P(None)),
        out_specs=(row_spec, row_spec),
        check_vma=False,
    )
```

```python
import functools

import jax
import jax.numpy as jnp
from jax import lax
from jax.experimental import pallas as pl
from jax.experimental.pallas import tpu as pltpu
from jax.sharding import PartitionSpec as P

EPS = 1e-5
MESH = pl.DeviceIdType.MESH
TILE = 128
LANE = 128
STEP = 256
COLS = 512
ROWS = 16


def dot_nt(a, b):
    return lax.dot_general(a, b, (((1,), (1,)), ((), ())), preferred_element_type=jnp.float32)


def gated(gate_val, up_val):
    return (jax.nn.silu(gate_val) * up_val).astype(jnp.bfloat16)


def mlp_kernel(
    tp, x_hbm, wg_hbm, wu_hbm, wd_hbm, res_hbm, gain_ref, h_ref, n_ref,
    wg, wu, wt, wt_t, wd, xbuf, gbuf, own, dsend, drecv, rrecv, res,
    w_sem, x_sem, res_sem, ds_sem, dr_sem, rs_sem, rr_sem,
):
    rows, width = res_hbm.shape
    hid = wg_hbm.shape[0]
    main = hid // LANE * LANE
    tail = hid - main
    chips = tp // 2
    subs = rows // TILE
    sends = (chips - 1) * subs
    total = chips * subs

    me = lax.axis_index("tp")
    chip, core = me // 2, lax.rem(me, 2)
    step_dir = 1 - 2 * core
    partner = me + step_dir
    ahead = 2 * lax.rem(chip + step_dir + chips, chips) + core
    behind = 2 * lax.rem(chip - step_dir + chips, chips) + core

    def x_copies(t, slot):
        s, j = t // subs + 1, lax.rem(t, subs)
        theirs = 2 * lax.rem(chip + s * step_dir + 2 * chips, chips) + (1 - core)
        mine = 2 * lax.rem(chip - s * step_dir + 2 * chips, chips) + core
        return [
            pltpu.make_async_copy(
                x_hbm.at[pl.ds(pl.multiple_of(dest * rows + j * TILE, TILE), TILE), :],
                xbuf.at[slot, pl.ds(i * TILE, TILE), :],
                x_sem.at[slot, i],
            )
            for i, dest in enumerate((theirs, mine))
        ]

    def d2d_copy(t):
        slot = lax.rem(t, 2)
        return pltpu.make_async_remote_copy(
            src_ref=dsend.at[slot], dst_ref=drecv.at[t], send_sem=ds_sem.at[slot], recv_sem=dr_sem.at[t],
            device_id={"tp": partner}, device_id_type=MESH,
        )

    def ring_copy(t):
        return pltpu.make_async_remote_copy(
            src_ref=drecv.at[t], dst_ref=rrecv.at[t], send_sem=rs_sem.at[t], recv_sem=rr_sem.at[t],
            device_id={"tp": ahead}, device_id_type=MESH,
        )

    for copy in x_copies(0, 0):
        copy.start()
    last = main // STEP
    tail_loads = [
        pltpu.make_async_copy(wg_hbm.at[pl.ds(main, tail), :], wt.at[pl.ds(0, tail), :], w_sem.at[0, last]),
        pltpu.make_async_copy(wu_hbm.at[pl.ds(main, tail), :], wt.at[pl.ds(LANE, tail), :], w_sem.at[1, last]),
    ]
    for copy in tail_loads:
        copy.start()
    up_steps = [(c, min(STEP, main - c)) for c in range(0, main, STEP)]
    gate_loads, up_loads = [], []
    for i, (c, n) in enumerate(up_steps):
        gate_loads.append(pltpu.make_async_copy(wg_hbm.at[pl.ds(c, n), :], wg.at[pl.ds(c, n), :], w_sem.at[0, i]))
        up_loads.append(pltpu.make_async_copy(wu_hbm.at[pl.ds(c, n), :], wu.at[pl.ds(c, n), :], w_sem.at[1, i]))
    down_loads = [pltpu.make_async_copy(wd_hbm, wd.at[pl.ds(0, hid), :], w_sem.at[2, 0])]
    res_copy = pltpu.make_async_copy(res_hbm, res, res_sem)
    half = len(up_steps) // 2
    for copy in gate_loads[:half] + up_loads[:half]:
        copy.start()

    barrier = pltpu.get_barrier_semaphore()
    for peer in (partner, ahead, behind):
        pl.semaphore_signal(barrier, inc=1, device_id={"tp": peer}, device_id_type=MESH)

    pad = jnp.zeros((LANE - tail, width), wd.dtype)
    wt[pl.ds(tail, LANE - tail), :] = pad
    wt[pl.ds(LANE + tail, LANE - tail), :] = pad
    wd[pl.ds(hid, LANE - tail), :] = pad

    def hidden_step(t, c, n):
        x = xbuf[lax.rem(t, 2)]
        gbuf[lax.rem(t, 2), :, c:c + n] = gated(dot_nt(x, wg[c:c + n, :]), dot_nt(x, wu[c:c + n, :]))

    def hidden_tail(t):
        for i in range(2):
            at = pl.ds(i * TILE, TILE)
            both = jnp.dot(xbuf[lax.rem(t, 2), at, :], wt_t[...], preferred_element_type=jnp.float32)
            gbuf[lax.rem(t, 2), at, main:main + LANE] = gated(both[:, :LANE], both[:, LANE:])

    def down_step(t, c):
        g = gbuf[lax.rem(t, 2)]
        y = jnp.dot(g, wd[:, c:c + COLS], preferred_element_type=jnp.float32).astype(jnp.bfloat16)
        dsend[lax.rem(t, 2), :, c:c + COLS] = y[:TILE]
        own[lax.rem(t, subs), :, c:c + COLS] = y[TILE:]

    def down_rows(t, c, i):
        g = gbuf[lax.rem(t, 2), pl.ds(i * TILE, TILE), :]
        y = jnp.dot(g, wd[:, c:c + COLS], preferred_element_type=jnp.float32).astype(jnp.bfloat16)
        if i == 0:
            dsend[lax.rem(t, 2), :, c:c + COLS] = y
        else:
            own[lax.rem(t, subs), :, c:c + COLS] = y

    def combine(t, first, part=0, parts=1):
        for r in range(part * TILE // parts, (part + 1) * TILE // parts, ROWS):
            for c in range(0, width, COLS):
                at = (pl.ds(r, ROWS), slice(c, c + COLS))
                both = own[lax.rem(t, subs), *at].astype(jnp.float32) + drecv[t, *at].astype(jnp.float32)
                if not first:
                    both = both + rrecv[t - subs, *at].astype(jnp.float32)
                drecv[t, *at] = both.astype(jnp.bfloat16)

    def finish_rows(j, r):
        at = pl.ds(r, ROWS)
        out_at = pl.ds(pl.multiple_of(j * TILE + r, ROWS), ROWS)
        y = own[j, at, :].astype(jnp.float32) + drecv[sends + j, at, :].astype(jnp.float32)
        y = y + rrecv[sends - subs + j, at, :].astype(jnp.float32)
        h = res[out_at, :].astype(jnp.float32) + y
        mean_sq = jnp.mean(h * h, axis=-1, keepdims=True)
        h_ref[out_at, :] = h.astype(jnp.bfloat16)
        n_ref[out_at, :] = (h * lax.rsqrt(mean_sq + EPS) * gain_ref[...].reshape(1, width)).astype(jnp.bfloat16)

    def wait_last(j):
        d2d_copy(sends + j).wait_recv()
        ring_copy(sends - subs + j).wait_recv()

    def early_tile(t, with_sum=True):
        for copy in x_copies(t + 2, lax.rem(t, 2)):
            copy.start()
        for copy in x_copies(t + 1, lax.rem(t + 1, 2)):
            copy.wait()

        d2d_copy(t).wait_send()
        if with_sum:
            d2d_copy(t - 1).wait_recv()
            combine(t - 1, True)
            ring_copy(t - 1).start()
        for c in range(0, width, COLS):
            down_step(t, c)
        d2d_copy(t).start()
        for c, n in up_steps:
            hidden_step(t + 1, c, n)
        hidden_tail(t + 1)

    def tile(t, with_sum, with_end, lag=2):
        @pl.when(t + 2 < total)
        def _():
            for copy in x_copies(t + 2, lax.rem(t, 2)):
                copy.start()

        for copy in x_copies(t + 1, lax.rem(t + 1, 2)):
            copy.wait()
        d2d_copy(t).wait_send()
        if with_sum:
            d2d_copy(t - lag).wait_recv()
            ring_copy(t - lag - subs).wait_recv()
        if with_end:
            wait_last(t - 2 - sends)
        for c in range(0, width, COLS):
            down_step(t, c)
        parts = len(up_steps)
        for i, (c, n) in enumerate(up_steps):
            hidden_step(t + 1, c, n)
            if with_sum:
                combine(t - lag, False, i, parts)
            if with_end:
                for r in range(i * TILE // parts, (i + 1) * TILE // parts, ROWS):
                    finish_rows(t - 2 - sends, r)
        hidden_tail(t + 1)
        if with_sum:
            ring_copy(t - lag).start()
        d2d_copy(t).start()

    for copy in x_copies(0, 0):
        copy.wait()
    for copy in gate_loads[half:] + up_loads[half:] + down_loads:
        copy.start()
    for copy in tail_loads:
        copy.wait()
    wt_t[...] = wt[...].T
    hidden_tail(0)
    for part in (range(half), range(half, len(up_steps))):
        for i in part:
            gate_loads[i].wait()
            up_loads[i].wait()
        for i in part:
            hidden_step(0, *up_steps[i])
    for copy in x_copies(1, 1):
        copy.start()
    for copy in down_loads:
        copy.wait()
    pl.semaphore_wait(barrier, 3)
    for c in range(0, width, COLS):
        down_rows(0, c, 0)
    d2d_copy(0).start()
    for copy in x_copies(2, 0):
        copy.start()
    for copy in x_copies(1, 1):
        copy.wait()
    for c in range(0, width, COLS):
        down_rows(0, c, 1)
    for c, n in up_steps[:half]:
        hidden_step(1, c, n)
    res_copy.start()
    d2d_copy(0).wait_recv()
    combine(0, True)
    ring_copy(0).start()
    for c, n in up_steps[half:]:
        hidden_step(1, c, n)
    hidden_tail(1)

    def early(t, carry):
        early_tile(t)
        return carry

    def with_sum(t, carry):
        tile(t, True, False)
        return carry

    def with_end(t, carry):
        tile(t, False, True)
        return carry

    for copy in x_copies(3, 1):
        copy.start()
    for copy in x_copies(2, 0):
        copy.wait()
    for c in range(0, width, COLS):
        down_rows(1, c, 0)
    d2d_copy(1).start()
    for c in range(0, width, COLS):
        down_rows(1, c, 1)
    for c, n in up_steps[:half]:
        hidden_step(2, c, n)
    d2d_copy(1).wait_recv()
    combine(1, True)
    ring_copy(1).start()
    for c, n in up_steps[half:]:
        hidden_step(2, c, n)
    hidden_tail(2)
    early_tile(2, False)
    lax.fori_loop(3, subs + 1, early, 0)
    tile(subs + 1, True, False, lag=1)
    tile(subs + 2, False, False)
    lax.fori_loop(subs + 3, sends + 2, with_sum, 0)
    res_copy.wait()
    lax.fori_loop(sends + 2, total - 1, with_end, 0)
    d2d_copy(total - 1).wait_send()
    for c in range(0, width, COLS):
        down_step(total - 1, c)
    d2d_copy(total - 1).start()

    def finish_tile(j, carry):
        wait_last(j)
        for r in range(0, TILE, ROWS):
            finish_rows(j, r)
        return carry

    lax.fori_loop(total - 3 - sends, subs, finish_tile, 0)

    for t in (total - 2, total - 1):
        d2d_copy(t).wait_send()
    for t in range(sends):
        ring_copy(t).wait_send()


def store_kernel(h_ref, n_ref, h_hbm, n_hbm, sem):
    rows = h_ref.shape[0] // 2
    copies = [
        pltpu.make_async_copy(src.at[pl.ds(i * rows, rows), :], dst.at[pl.ds(i * rows, rows), :], sem.at[k, i])
        for i in range(2)
        for k, (src, dst) in enumerate(((h_ref, h_hbm), (n_ref, n_hbm)))
    ]
    for copy in copies:
        copy.start()
    for copy in copies:
        copy.wait()


def solution(mesh):
    tp = mesh.shape["tp"]

    def local_block(x_in, w_gate, w_up, w_down, residual, norm_gain):
        rows, width = residual.shape
        hid = w_gate.shape[1]
        main = hid // LANE * LANE
        padded = main + LANE
        chips, subs = tp // 2, rows // TILE
        sends, total = (chips - 1) * subs, chips * subs
        bf16 = jnp.bfloat16
        any_spec = pl.BlockSpec(memory_space=pl.ANY)
        vmem_spec = pl.BlockSpec(memory_space=pltpu.VMEM)
        out = pltpu.VMEM((rows, width), bf16)
        flops = 6 * x_in.shape[0] * width * hid
        h_out, n_out = pl.pallas_call(
            functools.partial(mlp_kernel, tp),
            out_shape=(out, out),
            in_specs=[any_spec] * 5 + [vmem_spec],
            out_specs=(vmem_spec, vmem_spec),
            scratch_shapes=[
                pltpu.VMEM((main, width), bf16),
                pltpu.VMEM((main, width), bf16),
                pltpu.VMEM((2 * LANE, width), bf16),
                pltpu.VMEM((width, 2 * LANE), bf16),
                pltpu.VMEM((padded, width), bf16),
                pltpu.VMEM((2, 2 * TILE, width), bf16),
                pltpu.VMEM((2, 2 * TILE, padded), bf16),
                pltpu.VMEM((subs, TILE, width), bf16),
                pltpu.VMEM((2, TILE, width), bf16),
                pltpu.VMEM((total, TILE, width), bf16),
                pltpu.VMEM((sends, TILE, width), bf16),
                pltpu.VMEM((rows, width), bf16),
                pltpu.SemaphoreType.DMA((3, main // STEP + 2)),
                pltpu.SemaphoreType.DMA((2, 2)),
                pltpu.SemaphoreType.DMA,
                pltpu.SemaphoreType.DMA((2,)),
                pltpu.SemaphoreType.DMA((total,)),
                pltpu.SemaphoreType.DMA((sends,)),
                pltpu.SemaphoreType.DMA((sends,)),
            ],
            compiler_params=pltpu.CompilerParams(
                collective_id=0, has_side_effects=True, vmem_limit_bytes=56 * 2**20,
            ),
            cost_estimate=pl.CostEstimate(flops=flops, bytes_accessed=2 * x_in.size, transcendentals=0),
        )(x_in, w_gate.T, w_up.T, w_down, residual, norm_gain)
        stored = jax.ShapeDtypeStruct((rows, width), bf16)
        return pl.pallas_call(
            store_kernel,
            out_shape=(stored, stored),
            in_specs=[vmem_spec, vmem_spec],
            out_specs=(any_spec, any_spec),
            scratch_shapes=[pltpu.SemaphoreType.DMA((2, 2))],
            compiler_params=pltpu.CompilerParams(vmem_limit_bytes=2**20),
        )(pltpu.with_memory_space_constraint(h_out, pltpu.VMEM), pltpu.with_memory_space_constraint(n_out, pltpu.VMEM))

    row_spec = P(("data", "tp"), None)
    return jax.shard_map(
        local_block,
        mesh=mesh,
        in_specs=(P("data", None), P(None, "tp"), P(None, "tp"), P("tp", None), row_spec, P(None)),
        out_specs=(row_spec, row_spec),
        check_vma=False,
    )
```
